32 devices in a mesh: data: 32 (over z, y, x, core).
Axes of the slice: x: 2, y: 2, z: 4, core: 2. Of those that a mesh axis runs over, the one named last changes fastest.
Arguments:
- tokens: bfloat16 [16384, 512], P('data')
- d_logits: bfloat16 [16384, 32000], P('data')
- w_up: bfloat16 [2, 512, 1376], replicated
- w_down: bfloat16 [2, 1376, 512], replicated
- w_out: bfloat16 [512, 32000], replicated
- proj_up: bfloat16 [2, 512, 128], replicated
- proj_down: bfloat16 [2, 512, 128], replicated
- mom_up: float32 [2, 128, 1376], P(None, None, 'data')
- var_up: float32 [2, 128, 1376], P(None, None, 'data')
- mom_down: float32 [2, 1376, 128], P(None, 'data')
- var_down: float32 [2, 1376, 128], P(None, 'data')
- mom_out: float32 [512, 32000], P(None, 'data')
- var_out: float32 [512, 32000], P(None, 'data')
Outputs:
- output 1: bfloat16 [2, 512, 1376], replicated
- output 2: bfloat16 [2, 1376, 512], replicated
- output 3: bfloat16 [512, 32000], replicated
- output 4: float32 [2, 128, 1376], P(None, None, 'data')
- output 5: float32 [2, 128, 1376], P(None, None, 'data')
- output 6: float32 [2, 1376, 128], P(None, 'data')
- output 7: float32 [2, 1376, 128], P(None, 'data')
- output 8: float32 [512, 32000], P(None, 'data')
- output 9: float32 [512, 32000], P(None, 'data')
All inputs are finite; a program needn't handle non-finite values.
Results may differ from the reference program's by a relative error of at most 0.00412998.
Values are sent between devices in bfloat16 or wider.
A program may use at most 1 GiB of HBM per device.

```python
import jax
import jax.numpy as jnp

D = 512
FF = 1376
RANK = 128
VOCAB = 32000
TOKENS = 16384
LAYERS = 2
STEP = 4

BETA1 = 0.9
BETA2 = 0.999
EPS = 1e-8
LR = 0.02
ALPHA = 0.5
LR_HEAD = 0.01


def gelu_tanh(values):
    return jax.nn.gelu(values, approximate=True)


def adam_update(gradient, moment_one, moment_two):
    moment_one = BETA1 * moment_one + (1.0 - BETA1) * gradient
    moment_two = BETA2 * moment_two + (1.0 - BETA2) * gradient * gradient
    direction = (moment_one / (1.0 - BETA1 ** STEP)) / (jnp.sqrt(moment_two / (1.0 - BETA2 ** STEP)) + EPS)
    return moment_one, moment_two, direction


def setup_inputs(seed: int = 0) -> dict:
    subkeys = jax.random.split(jax.random.key(seed), 13)
    scale_up = 0.7 * (D / FF) ** 0.5
    scale_down = 0.85
    scale_out = 1.3 * (D / VOCAB) ** 0.5

    def normal(key_num, arr_dims, factor):
        return jax.random.normal(subkeys[key_num], arr_dims, jnp.float32) * factor

    def spread(key_num, arr_dims, factor):
        return jax.random.uniform(subkeys[key_num], arr_dims, jnp.float32, 0.5, 1.5) * factor

    return {
        'tokens': normal(0, (TOKENS, D), 1.0).astype(jnp.bfloat16),
        'd_logits': normal(1, (TOKENS, VOCAB), (D / (VOCAB * TOKENS)) ** 0.5).astype(jnp.bfloat16),
        'w_up': normal(2, (LAYERS, D, FF), D ** -0.5).astype(jnp.bfloat16),
        'w_down': normal(3, (LAYERS, FF, D), FF ** -0.5).astype(jnp.bfloat16),
        'w_out': normal(4, (D, VOCAB), D ** -0.5).astype(jnp.bfloat16),
        'proj_up': normal(5, (LAYERS, D, RANK), D ** -0.5).astype(jnp.bfloat16),
        'proj_down': normal(6, (LAYERS, D, RANK), D ** -0.5).astype(jnp.bfloat16),
        'mom_up': normal(7, (LAYERS, RANK, FF), 0.1 * scale_up),
        'var_up': spread(8, (LAYERS, RANK, FF), 0.003 * scale_up ** 2),
        'mom_down': normal(9, (LAYERS, FF, RANK), 0.1 * scale_down),
        'var_down': spread(10, (LAYERS, FF, RANK), 0.003 * scale_down ** 2),
        'mom_out': normal(11, (D, VOCAB), 0.1 * scale_out),
        'var_out': spread(12, (D, VOCAB), 0.003 * scale_out ** 2),
    }


def layer_forward(hidden, w_first, w_second):
    pre_act = jnp.dot(hidden, w_first, preferred_element_type=jnp.float32).astype(jnp.bfloat16)
    post_act = gelu_tanh(pre_act.astype(jnp.float32)).astype(jnp.bfloat16)
    new_hidden = (hidden.astype(jnp.float32) + jnp.dot(post_act, w_second, preferred_element_type=jnp.float32)).astype(jnp.bfloat16)
    return new_hidden, pre_act, post_act


def reference(tokens, d_logits, w_up, w_down, w_out, proj_up, proj_down, mom_up, var_up, mom_down, var_down, mom_out, var_out):
    hidden = tokens
    saved_acts = []
    for layer_idx in range(LAYERS):
        new_hidden, pre_act, post_act = layer_forward(hidden, w_up[layer_idx], w_down[layer_idx])
        saved_acts.append((hidden, pre_act, post_act))
        hidden = new_hidden
    grad_head = jnp.dot(hidden.T, d_logits, preferred_element_type=jnp.float32)
    grad_hidden = jnp.dot(d_logits, w_out.T, preferred_element_type=jnp.float32).astype(jnp.bfloat16)
    results = []
    for layer_idx in reversed(range(LAYERS)):
        hidden_in, pre_act, post_act = saved_acts[layer_idx]
        grad_down = jnp.dot(post_act.T, grad_hidden, preferred_element_type=jnp.float32)
        d_post = jnp.dot(grad_hidden, w_down[layer_idx].T, preferred_element_type=jnp.float32)
        gelu_pull = jax.vjp(gelu_tanh, pre_act.astype(jnp.float32))[1]
        d_pre = gelu_pull(d_post)[0].astype(jnp.bfloat16)
        grad_up = jnp.dot(hidden_in.T, d_pre, preferred_element_type=jnp.float32)
        if layer_idx > 0:
            grad_hidden = (grad_hidden.astype(jnp.float32) + jnp.dot(d_pre, w_up[layer_idx].T, preferred_element_type=jnp.float32)).astype(jnp.bfloat16)
        low_up = jnp.dot(proj_up[layer_idx].astype(jnp.float32).T, grad_up, preferred_element_type=jnp.float32)
        low_down = jnp.dot(grad_down, proj_down[layer_idx].astype(jnp.float32), preferred_element_type=jnp.float32)
        m_up, v_up, dir_up = adam_update(low_up, mom_up[layer_idx], var_up[layer_idx])
        m_down, v_down, dir_down = adam_update(low_down, mom_down[layer_idx], var_down[layer_idx])
        step_up = jnp.dot(proj_up[layer_idx], dir_up.astype(jnp.bfloat16), preferred_element_type=jnp.float32)
        step_down = jnp.dot(dir_down.astype(jnp.bfloat16), proj_down[layer_idx].T, preferred_element_type=jnp.float32)
        new_up = (w_up[layer_idx].astype(jnp.float32) - LR * ALPHA * step_up).astype(jnp.bfloat16)
        new_down = (w_down[layer_idx].astype(jnp.float32) - LR * ALPHA * step_down).astype(jnp.bfloat16)
        results.append((new_up, new_down, m_up, v_up, m_down, v_down))
    results = results[::-1]
    m_out, v_out, dir_out = adam_update(grad_head, mom_out, var_out)
    w_out_new = (w_out.astype(jnp.float32) - LR_HEAD * dir_out).astype(jnp.bfloat16)
    return (jnp.stack([entry[0] for entry in results]),
            jnp.stack([entry[1] for entry in results]),
            w_out_new,
            jnp.stack([entry[2] for entry in results]),
            jnp.stack([entry[3] for entry in results]),
            jnp.stack([entry[4] for entry in results]),
            jnp.stack([entry[5] for entry in results]),
            m_out,
            v_out)
```

```python
import functools

import jax
import jax.numpy as jnp
from jax import lax
from jax.experimental import pallas as pl
from jax.experimental.pallas import tpu as pltpu
from jax.experimental.layout import Layout, with_layout_constraint
from jax.sharding import PartitionSpec as P

BETA1 = 0.9
BETA2 = 0.999
EPS = 1e-8
STEP = 4
LR = 0.02
ALPHA = 0.5
LR_HEAD = 0.01
DATA_AXIS = 'data'
DEVICES = 32
SHARD = 1000
HIDDEN = 512
TOKENS = 512
LOW = 43
CHUNKS = ((0, 256, 'x'), (256, 256, 'y'), (512, 256, 'x'), (768, 232, 'y'))
PAIRS = ((0, 1), (2, 3))


def position(index):
    return index >> 3, (index >> 2) & 1, (index >> 1) & 1, index & 1


def permutation(dz=0, dy=0, dx=0, dc=0):
    pairs = []
    for source in range(DEVICES):
        z, y, x, c = position(source)
        target = (((z ^ dz) * 2 + (y ^ dy)) * 2 + (x ^ dx)) * 2 + (c ^ dc)
        pairs.append((source, target))
    return pairs


def send(values, **move):
    return lax.ppermute(values, DATA_AXIS, permutation(**move))


def along(axis, core=0):
    return {'dx': int(axis == 'x'), 'dy': int(axis == 'y'), 'dc': core}


def padded(width):
    return -(-width // 128) * 128


def gelu_tanh(values):
    return jax.nn.gelu(values, approximate=True)


def adam_update(gradient, moment_one, moment_two):
    moment_one = BETA1 * moment_one + (1.0 - BETA1) * gradient
    moment_two = BETA2 * moment_two + (1.0 - BETA2) * gradient * gradient
    direction = (moment_one / (1.0 - BETA1 ** STEP)) / (jnp.sqrt(moment_two / (1.0 - BETA2 ** STEP)) + EPS)
    return moment_one, moment_two, direction


def relative(owner, me, first):
    z, y, x, c = position(owner)
    mz, my, mx, mc = position(me)
    rx, ry = mx ^ x, my ^ y
    a, b = (rx, ry) if first == 'x' else (ry, rx)
    dz = mz ^ z
    return a, mc ^ c, (dz >> 1) | ((dz & 1) << 1), b


def split_kernel(chunks, me_ref, logits_ref, *out_refs):
    me = me_ref[0]
    for (start, width, first), out_ref in zip(chunks, out_refs):
        for owner in range(DEVICES):
            a, core, zrel, b = relative(owner, me, first)
            slot = ((a * 2 + core) * 4 + zrel) * 2 + b
            base = owner * SHARD + start
            out_ref[slot, :, :width] = logits_ref[:, base:base + width]
            if width % 128:
                out_ref[slot, :, width:] = jnp.zeros((out_ref.shape[1], padded(width) - width), out_ref.dtype)


def split_columns(me, d_logits, chunks):
    rows = 32
    return pl.pallas_call(
        functools.partial(split_kernel, chunks),
        grid_spec=pltpu.PrefetchScalarGridSpec(
            num_scalar_prefetch=1,
            grid=(TOKENS // rows,),
            in_specs=[pl.BlockSpec((rows, DEVICES * SHARD), lambda i, s: (i, 0))],
            out_specs=[pl.BlockSpec((DEVICES, rows, padded(width)), lambda i, s: (0, i, 0)) for _, width, _ in chunks],
        ),
        out_shape=[jax.ShapeDtypeStruct((DEVICES, TOKENS, padded(width)), jnp.bfloat16) for _, width, _ in chunks],
        cost_estimate=pl.CostEstimate(flops=0, bytes_accessed=50_000_000, transcendentals=0),
    )(me, d_logits)


def partial_kernel(width, d0, d1, d2, d3, h0, h1, h2, h3, keep_ref, send_ref):
    for b, out_ref in ((0, keep_ref), (1, send_ref)):
        total = None
        for d_ref, h_ref in ((d0, h0), (d1, h1), (d2, h2), (d3, h3)):
            part = lax.dot_general(d_ref[b], h_ref[...], (((0,), (0,)), ((), ())), preferred_element_type=jnp.float32)
            total = part if total is None else total + part
        out_ref[0] = total[:width]


def partial_gradient(width, pieces, hiddens):
    lanes = padded(width)
    piece = pl.BlockSpec((2, TOKENS, lanes), lambda i: (i, 0, 0))
    whole = pl.BlockSpec((TOKENS, HIDDEN), lambda i: (0, 0))
    out = pl.BlockSpec((1, width, HIDDEN), lambda i: (i, 0, 0))
    shape = jax.ShapeDtypeStruct((4, width, HIDDEN), jnp.float32)
    return pl.pallas_call(
        functools.partial(partial_kernel, width),
        grid=(4,),
        in_specs=[piece] * 4 + [whole] * 4,
        out_specs=[out, out],
        out_shape=[shape, shape],
        cost_estimate=pl.CostEstimate(flops=2 * 8 * lanes * 2048 * 512, bytes_accessed=14_000_000, transcendentals=0),
    )(*pieces, *hiddens)


def join_kernel(me_ref, *refs):
    me = me_ref[0]
    out_ref = refs[-1]
    for (start, width, first), in_ref in zip(CHUNKS, refs[:-2]):
        for owner in range(DEVICES):
            a, core, zrel, b = relative(owner, me, first)
            slot = ((core * 2 + a) * 2 + b) * 4 + zrel
            base = owner * SHARD + start
            out_ref[:, base:base + width] = in_ref[slot]
    start = CHUNKS[PAIRS[-1][0]][0]
    for owner in range(DEVICES):
        out_ref[:, owner * SHARD + start:(owner + 1) * SHARD] = refs[-2][owner]


def join_columns(me, gathered):
    rows = 64
    return pl.pallas_call(
        join_kernel,
        grid_spec=pltpu.PrefetchScalarGridSpec(
            num_scalar_prefetch=1,
            grid=(HIDDEN // rows,),
            in_specs=[pl.BlockSpec((DEVICES, rows, part.shape[2]), lambda i, s: (0, i, 0)) for part in gathered],
            out_specs=pl.BlockSpec((rows, DEVICES * SHARD), lambda i, s: (i, 0)),
        ),
        out_shape=jax.ShapeDtypeStruct((HIDDEN, DEVICES * SHARD), jnp.bfloat16),
        cost_estimate=pl.CostEstimate(flops=0, bytes_accessed=67_000_000, transcendentals=0),
    )(me, *gathered)


def forward(tokens, w_up, w_down):
    hidden = tokens
    saved = []
    for layer in range(w_up.shape[0]):
        pre_act = jnp.dot(hidden, w_up[layer], preferred_element_type=jnp.float32).astype(jnp.bfloat16)
        post_act = gelu_tanh(pre_act.astype(jnp.float32)).astype(jnp.bfloat16)
        saved.append((hidden, pre_act, post_act))
        hidden = (hidden.astype(jnp.float32) + jnp.dot(post_act, w_down[layer], preferred_element_type=jnp.float32)).astype(jnp.bfloat16)
    return hidden, saved


def projected_gradients(saved, grad_hidden, w_up, w_down, proj_up, proj_down):
    ups = [None] * 2
    downs = [None] * 2
    for layer in (1, 0):
        hidden_in, pre_act, post_act = saved[layer]
        grad_down = jnp.einsum('tf,td->fd', post_act, grad_hidden, preferred_element_type=jnp.float32)
        d_post = jnp.einsum('td,fd->tf', grad_hidden, w_down[layer], preferred_element_type=jnp.float32)
        d_pre = jax.vjp(gelu_tanh, pre_act.astype(jnp.float32))[1](d_post)[0].astype(jnp.bfloat16)
        grad_up = jnp.einsum('td,tf->df', hidden_in, d_pre, preferred_element_type=jnp.float32)
        ups[layer] = jnp.einsum('dr,df->fr', proj_up[layer].astype(jnp.float32), grad_up, preferred_element_type=jnp.float32)
        downs[layer] = jnp.einsum('fd,dr->fr', grad_down, proj_down[layer].astype(jnp.float32), preferred_element_type=jnp.float32)
        if layer > 0:
            grad_hidden = (grad_hidden.astype(jnp.float32) + jnp.einsum('tf,df->td', d_pre, w_up[layer], preferred_element_type=jnp.float32)).astype(jnp.bfloat16)
    return jnp.concatenate(ups + downs, axis=1)


def scatter_low(low):
    low = jnp.pad(low.reshape(DEVICES, LOW, 4 * 128), ((0, 0), (0, 48 - LOW), (0, 0)))
    return lax.psum_scatter(low.reshape(DEVICES * 48, 4 * 128), DATA_AXIS, scatter_dimension=0, tiled=True)[:LOW]


def local_step(tokens, d_logits, w_up, w_down, w_out, proj_up, proj_down, mom_up, var_up, mom_down, var_down, mom_out, var_out):
    index = lax.axis_index(DATA_AXIS)
    me = index.reshape(1).astype(jnp.int32)

    cut = list(split_columns(me, d_logits, [CHUNKS[s] for s in PAIRS[0]]))
    tokens, _ = lax.optimization_barrier((tokens, cut[0]))
    hidden, saved = forward(tokens, w_up, w_down)
    near = {(axis, 0): send(hidden, **along(axis)) for axis in ('x', 'y')}
    near_core = send(hidden, dc=1)
    grad_hidden = jnp.einsum('tv,dv->td', d_logits, w_out, preferred_element_type=jnp.float32).astype(jnp.bfloat16)
    low = projected_gradients(saved, grad_hidden, w_up, w_down, proj_up, proj_down)
    for pair in PAIRS[1:]:
        later, _ = lax.optimization_barrier((d_logits, low))
        cut += split_columns(me, later, [CHUNKS[s] for s in pair])
    near, cut[2:] = lax.optimization_barrier((near, cut[2:]))
    near.update({(axis, 1): send(near[axis, 0], dc=1) for axis in ('x', 'y')})

    def wide(up, down):
        return jnp.concatenate([up[0].T, up[1].T, down[0], down[1]], axis=1)

    low_sum = scatter_low(low)
    own_out = lax.dynamic_slice_in_dim(w_out, index * SHARD, SHARD, axis=1)
    own_mom, own_var = mom_out.T, var_out.T
    gates = None
    pending = None
    firsts, seconds = [], []

    def finish(pair, kept, last):
        parts = {}
        for s in pair:
            start, width, _ = CHUNKS[s]
            total = kept[s][0] + last[s]
            m_out, v_out, direction = lax.optimization_barrier(
                adam_update(total, own_mom[start:start + width], own_var[start:start + width]))
            firsts.append(m_out)
            seconds.append(v_out)
            change = with_layout_constraint(LR_HEAD * direction, Layout(major_to_minor=(0, 1)))
            part = (own_out[:, start:start + width].astype(jnp.float32) - change.T).astype(jnp.bfloat16)
            parts[s] = with_layout_constraint(part, Layout(major_to_minor=(0, 1)))
        return parts

    for number, pair in enumerate(PAIRS):
        received, coming, keeps = {}, {}, {}
        for s in pair:
            first = CHUNKS[s][2]
            core, far, far_core = (cut[s][8 * k:8 * k + 8] for k in (1, 2, 3))
            if number:
                far, _ = lax.optimization_barrier((far, gates[0]))
                far_core, _ = lax.optimization_barrier((far_core, gates[1]))
            received[s] = (cut[s], send(core, dc=1), send(far, **along(first)), send(far_core, **along(first, 1)))
        if number:
            received, _ = lax.optimization_barrier((received, pending))
            kept = {s: before[s] + pending[s] for s in pending}
            last = {s: send(kept[s][1], dz=2) for s in pending}
            parts = finish(PAIRS[number - 1], kept, last)
            halves = {s: jnp.stack([parts[s], send(parts[s], dz=2)]) for s in parts}
            lines = {s: jnp.concatenate([halves[s], send(halves[s], dz=1)]) for s in parts}
        else:
            received = lax.optimization_barrier(received)
        for s in pair:
            first = CHUNKS[s][2]
            second = 'y' if first == 'x' else 'x'
            hiddens = (hidden, near_core, near[first, 0], near[first, 1])
            keeps[s], away = partial_gradient(CHUNKS[s][1], received[s], hiddens)
            coming[s] = send(away, **along(second))
        gates = ([received[s][3] for s in pair], coming)
        if number:
            coming, lines, low_all = lax.optimization_barrier((coming, lines, low_all))
            seconds_in, firsts_in = {}, {}
            for s in lines:
                first = CHUNKS[s][2]
                seconds_in[s] = send(lines[s], **along('y' if first == 'x' else 'x'))
                firsts_in[s] = send(lines[s], **along(first))
        if not number:
            coming, low_sum = lax.optimization_barrier((coming, low_sum))
            low_first, low_second, low_dir = adam_update(low_sum, wide(mom_up, mom_down), wide(var_up, var_down))
            low_all = lax.all_gather(jnp.pad(low_dir.astype(jnp.bfloat16), ((0, 48 - LOW), (0, 0))), DATA_AXIS, axis=0)
        before = {s: keeps[s][:2] + coming[s][:2] for s in pair}
        pending = {s: send(keeps[s][2:] + coming[s][2:], dz=1) for s in pair}
    for s, l in zip(pending, lines):
        pending[s], seconds_in[l], firsts_in[l] = lax.optimization_barrier((pending[s], seconds_in[l], firsts_in[l]))
    kept = {s: before[s] + pending[s] for s in pending}
    last = {s: send(kept[s][1], dz=2) for s in pending}
    groups = {s: [lines[s], seconds_in[s], firsts_in[s], send(seconds_in[s], **along(CHUNKS[s][2]))] for s in lines}
    last, groups = lax.optimization_barrier((last, groups))
    parts = finish(PAIRS[-1], kept, last)
    block = jnp.concatenate([parts[s] for s in PAIRS[-1]], axis=1)
    block = with_layout_constraint(block, Layout(major_to_minor=(0, 1)))
    tail = lax.all_gather(block, DATA_AXIS, axis=0)
    gathered = [jnp.concatenate(groups[s] + [send(values, dc=1) for values in groups[s]]) for s in groups]
    low_dirs = low_all[:, :LOW].reshape(DEVICES * LOW, 4 * 128)
    ups, downs = [], []
    for layer in range(2):
        dir_up = low_dirs[:, 128 * layer:128 * (layer + 1)]
        dir_down = low_dirs[:, 128 * (layer + 2):128 * (layer + 3)]
        step_up = jnp.einsum('dr,fr->df', proj_up[layer], dir_up, preferred_element_type=jnp.float32)
        step_down = jnp.einsum('fr,dr->fd', dir_down, proj_down[layer], preferred_element_type=jnp.float32)
        ups.append((w_up[layer].astype(jnp.float32) - LR * ALPHA * step_up).astype(jnp.bfloat16))
        downs.append((w_down[layer].astype(jnp.float32) - LR * ALPHA * step_down).astype(jnp.bfloat16))

    def narrow(values):
        up = jnp.stack([values[:, 0:128].T, values[:, 128:256].T])
        down = jnp.stack([values[:, 256:384], values[:, 384:512]])
        return up, down

    m_up, m_down = narrow(low_first)
    v_up, v_down = narrow(low_second)

    w_up_new, w_down_new, gathered, tail = lax.optimization_barrier((jnp.stack(ups), jnp.stack(downs), gathered, tail))
    w_out_new = join_columns(me, [*gathered, tail])
    return (w_up_new, w_down_new, w_out_new, m_up, v_up, m_down, v_down,
            jnp.concatenate(firsts).T, jnp.concatenate(seconds).T)


def solution(mesh):
    row_spec = P(DATA_AXIS, None)
    whole = P()
    up_spec = P(None, None, DATA_AXIS)
    down_spec = P(None, DATA_AXIS, None)
    head_spec = P(None, DATA_AXIS)
    in_specs = (row_spec, row_spec, whole, whole, whole, whole, whole, up_spec, up_spec, down_spec, down_spec, head_spec, head_spec)
    out_specs = (whole, whole, whole, up_spec, up_spec, down_spec, down_spec, head_spec, head_spec)
    return jax.shard_map(local_step, mesh=mesh, in_specs=in_specs, out_specs=out_specs, check_vma=False)
```
